32 devices in a mesh: ctx: 16 (over z, x, core), shard: 2 (over y).
Axes of the slice: x: 2, y: 2, z: 4, core: 2. Of those that a mesh axis runs over, the one named last changes fastest.
Arguments:
- tokens: bfloat16 [2, 2048, 1024], P('shard', 'ctx'), may hold values from -64 to 64
- lengths: int32 [2], P('shard'), may hold values from 512 to 2048
- positions: int32 [2, 2048], P('shard', 'ctx'), may hold values from 0 to 1023, as said below
- w_qkv: bfloat16 [1024, 3072], P('shard'), may hold values from -6 to 6
- w_out: bfloat16 [1024, 1024], P('shard'), may hold values from -6 to 6
- w_in: bfloat16 [1024, 5248], P('shard'), may hold values from -0.1875 to 0.1875
- w_down: bfloat16 [2624, 1024], P('shard'), may hold values from -0.125 to 0.125
- gain_attn: bfloat16 [1024], P('shard'), may hold values from 0.25 to 1.75
- gain_mlp: bfloat16 [1024], P('shard'), may hold values from 0.25 to 1.75
- cotangent: bfloat16 [2, 2048, 1024], P('shard', 'ctx'), may hold values from -6 to 6
Outputs:
- output: bfloat16 [2, 2048, 1024], P('shard', 'ctx')
- grad_tokens: float32 [2, 2048, 1024], P('shard', 'ctx')
- grad_qkv: float32 [1024, 3072], P('shard')
- grad_out: float32 [1024, 1024], P('shard')
- grad_in: float32 [1024, 5248], P('shard')
- grad_down: float32 [2624, 1024], P('shard')
- grad_gain_attn: float32 [1024], P('shard')
- grad_gain_mlp: float32 [1024], P('shard')
The draws below stay inside these ranges and needn't reach their ends.
Inputs may be any that keep to these rules, and one draw needn't show every extreme that they name: Within each sequence positions count up by one from 0 inside documents that follow each other; the first min(1024, 1024) tokens of a sequence form one document, and every token whose index is a multiple of min(1024, 1024) starts a document. The first lengths tokens of a sequence are valid keys, the rest are padding.
All inputs are finite; a program needn't handle non-finite values.
Results may differ from the reference program's by a relative error of at most 0.015.
Values may be sent and summed in bfloat16 or wider, within the bound.
A program may use at most 384 MiB of HBM per device.

```python
import math
import jax
import jax.numpy as jnp
from jax import lax

D = 1024
HEADS = 16
FF = 2624
HEAD_DIM = 64
LEN = 2048
SEQS = 2


def draw_positions(key, part):
    period = min(LEN // 2, 1024)
    index = jnp.broadcast_to(jnp.arange(LEN, dtype=jnp.int32)[None, :], (SEQS, LEN))
    random_marks = (jax.random.randint(key, (SEQS, LEN), 0, 16) == 0) & (index > period)
    marks = random_marks | (index % period == 0)
    starts = jnp.where(marks, index, 0)
    return index - lax.cummax(starts, axis=1)


def draw_tokens(key, part):
    return jnp.clip(jax.random.normal(jax.random.fold_in(key, 11), (SEQS, LEN, D), jnp.float32), -6.0, 6.0).astype(jnp.bfloat16)


def draw_w_qkv(key, part):
    return (jnp.clip(jax.random.normal(jax.random.fold_in(key, 24), (D, 3 * D), jnp.float32), -6.0, 6.0) * D ** (-0.5)).astype(jnp.bfloat16)


def levels(own_key, dims, cuts, low, largest):
    def one(dim, shards_of):
        heights = jax.random.uniform(jax.random.fold_in(jax.random.fold_in(own_key, 6), dim), (shards_of,), jnp.float32, low / len(cuts), largest / len(cuts))
        return jnp.repeat(jnp.exp(heights), dims[dim] // shards_of).reshape((-1,) + (1,) * (len(dims) - dim - 1))

    factor_of = one(*cuts[0])
    for cut in cuts[1:]:
        factor_of = factor_of * one(*cut)
    return factor_of


def centred(own_key, shape, scale, most, pieces=(), held_as=jnp.bfloat16):
    result = scale * jax.random.normal(own_key, shape, jnp.float32)
    if pieces:
        result = result * levels(own_key, shape, pieces, -0.22, 0.18)
    return jnp.clip(result, -most, most).astype(held_as)


def setup_inputs(seed: int = 0) -> dict:
    key_list = jax.random.split(jax.random.key(seed), 11)
    return {
        "tokens": draw_tokens(jax.random.fold_in(key_list[10], 71), 0),
        "lengths": jax.random.randint(key_list[1], (SEQS,), LEN // 4, LEN + 1).astype(jnp.int32),
        "positions": draw_positions(jax.random.fold_in(key_list[10], 71), 0),
        "w_qkv": draw_w_qkv(jax.random.fold_in(key_list[10], 71), 0),
        "w_out": centred(key_list[4], (D, D), (((LEN // 8) ** 0.5) * (D ** -0.5)), 6.0, ((0, 2),)),
        "w_in": centred(key_list[5], (D, 2 * FF), D ** -0.5, 0.1875, ((0, 2),)),
        "w_down": centred(key_list[6], (FF, D), FF ** -0.5, 0.125, ((0, 2),)),
        "gain_attn": jnp.clip(1.0 + 0.15 * jax.random.normal(key_list[7], (D,), jnp.float32), 0.25, 1.75).astype(jnp.bfloat16),
        "gain_mlp": jnp.clip(1.0 + 0.15 * jax.random.normal(key_list[8], (D,), jnp.float32), 0.25, 1.75).astype(jnp.bfloat16),
        "cotangent": centred(key_list[9], (SEQS, LEN, D), 1.0, 6.0, ((0, 2), (1, 16))),
    }


eps = 1e-05
theta_base = 160000.0
masked_score = -1e+30

def rounded(value):
    return lax.optimization_barrier(value.astype(jnp.bfloat16)).astype(jnp.float32)

def layer_norm(value, gain):
    mean = lax.optimization_barrier(jnp.mean(value, axis=-1, keepdims=True))
    centered = value - mean
    rstd = lax.rsqrt(lax.optimization_barrier(jnp.mean(centered * centered, axis=-1, keepdims=True)) + eps)
    normed = centered * rstd
    return (normed * gain.astype(jnp.float32), normed, rstd)

def norm_back(grad_h, normed, rstd, gain):
    grad_n = grad_h * gain.astype(jnp.float32)
    grad_gain = lax.optimization_barrier(jnp.sum(grad_h * normed, axis=0))
    grad_x = rstd * (grad_n - lax.optimization_barrier(jnp.mean(grad_n, axis=-1, keepdims=True)) - normed * lax.optimization_barrier(jnp.mean(grad_n * normed, axis=-1, keepdims=True)))
    return (grad_x, grad_gain)

def rope_tables(pos_ids):
    half = HEAD_DIM // 2
    inverse = theta_base ** (-(jnp.arange(half, dtype=jnp.float32) * (2.0 / HEAD_DIM)))
    angles = pos_ids.astype(jnp.float32)[:, None] * inverse[None, :]
    return (jnp.cos(angles)[:, None, :], jnp.sin(angles)[:, None, :])

def rotate(value, cosv, sinv):
    half = value.shape[-1] // 2
    first, second = (value[..., :half], value[..., half:])
    return jnp.concatenate([first * cosv - second * sinv, second * cosv + first * sinv], axis=-1)

def unrotate(value, cosv, sinv):
    half = value.shape[-1] // 2
    first, second = (value[..., :half], value[..., half:])
    return jnp.concatenate([first * cosv + second * sinv, second * cosv - first * sinv], axis=-1)

def gelu_parts(value):
    cdf = 0.5 * (1.0 + jax.scipy.special.erf(value * 0.7071067811865476))
    dens = jnp.exp(-0.5 * value * value) * 0.3989422804014327
    return (value * cdf, cdf + value * dens)

def one_sequence(seq_x, length, pos_ids, w_qkv, w_out, w_in, w_down, gain_attn, gain_mlp, seq_cot):
    rows = seq_x.shape[0]
    scale = HEAD_DIM ** (-0.5)
    hidden_in = seq_x.astype(jnp.float32)
    h1, n1, r1 = layer_norm(hidden_in, gain_attn)
    hb1 = h1.astype(jnp.bfloat16)
    qkv = jnp.dot(hb1, w_qkv, preferred_element_type=jnp.float32)
    cosv, sinv = rope_tables(pos_ids)
    q = rotate(qkv[:, :D].reshape(rows, HEADS, HEAD_DIM), cosv, sinv)
    k = rotate(qkv[:, D:2 * D].reshape(rows, HEADS, HEAD_DIM), cosv, sinv)
    v = qkv[:, 2 * D:].reshape(rows, HEADS, HEAD_DIM)
    qf, kf, vf = (rounded(q), rounded(k), rounded(v))
    valid = jnp.arange(rows) < length
    block = math.gcd(rows, 512)
    count = rows // block
    qblocks = qf.reshape(count, block, HEADS, HEAD_DIM)

    def forward_block(qblk):
        s = jnp.einsum('qhd,khd->hqk', qblk, kf) * scale
        s = jnp.where(valid, s, masked_score)
        top = lax.optimization_barrier(jnp.max(s, axis=-1))
        e = jnp.where(valid, jnp.exp(s - top[:, :, None]), 0.0)
        tot = lax.optimization_barrier(jnp.sum(e, axis=-1))
        acc = jnp.einsum('hqk,khd->qhd', rounded(e), vf)
        return (acc / jnp.transpose(tot)[:, :, None], top + jnp.log(tot))
    o_blocks, lse_blocks = lax.map(forward_block, qblocks)
    o = o_blocks.reshape(rows, HEADS, HEAD_DIM)
    ob = o.reshape(rows, D).astype(jnp.bfloat16)
    mid = hidden_in + jnp.dot(ob, w_out, preferred_element_type=jnp.float32)
    h2, n2, r2 = layer_norm(mid, gain_mlp)
    hb2 = h2.astype(jnp.bfloat16)
    u = jnp.dot(hb2, w_in, preferred_element_type=jnp.float32)
    inp, gate = (u[:, :FF], u[:, FF:])
    gel, dgel = gelu_parts(inp)
    act = (gel * gate).astype(jnp.bfloat16)
    out = (mid + jnp.dot(act, w_down, preferred_element_type=jnp.float32)).astype(jnp.bfloat16)
    cot = seq_cot.astype(jnp.float32)
    grad_down = jnp.dot(act.T, seq_cot, preferred_element_type=jnp.float32)
    d_act = jnp.dot(seq_cot, w_down.T, preferred_element_type=jnp.float32)
    d_u = jnp.concatenate([d_act * gate * dgel, d_act * gel], axis=1).astype(jnp.bfloat16)
    grad_in = jnp.dot(hb2.T, d_u, preferred_element_type=jnp.float32)
    d_h2 = jnp.dot(d_u, w_in.T, preferred_element_type=jnp.float32)
    d_x2, grad_g2 = norm_back(d_h2, n2, r2, gain_mlp)
    d_mid = cot + d_x2
    d_mid_b = d_mid.astype(jnp.bfloat16)
    grad_out = jnp.dot(ob.T, d_mid_b, preferred_element_type=jnp.float32)
    d_att = rounded(jnp.dot(d_mid_b, w_out.T, preferred_element_type=jnp.float32)).reshape(rows, HEADS, HEAD_DIM)
    delta = lax.optimization_barrier(jnp.sum(d_att * o, axis=-1))
    do_blocks = d_att.reshape(count, block, HEADS, HEAD_DIM)
    delta_blocks = delta.reshape(count, block, HEADS)

    def backward_block(carry, inputs):
        dk, dv = carry
        qblk, doblk, lseblk, deltablk = inputs
        s = jnp.einsum('qhd,khd->hqk', qblk, kf) * scale
        p = jnp.where(valid, jnp.exp(s - lseblk[:, :, None]), 0.0)
        dp = jnp.einsum('qhd,khd->hqk', doblk, vf)
        ds = rounded(p * (dp - jnp.transpose(deltablk)[:, :, None]))
        dq = jnp.einsum('hqk,khd->qhd', ds, kf)
        dv = dv + jnp.einsum('hqk,qhd->khd', rounded(p), doblk)
        dk = dk + jnp.einsum('hqk,qhd->khd', ds, qblk)
        return ((dk, dv), dq)
    zero = jnp.zeros((rows, HEADS, HEAD_DIM), jnp.float32)
    (dk, dv), dq_blocks = lax.scan(backward_block, (zero, zero), (qblocks, do_blocks, lse_blocks, delta_blocks))
    dq = unrotate(dq_blocks.reshape(rows, HEADS, HEAD_DIM) * scale, cosv, sinv)
    dk = unrotate(dk * scale, cosv, sinv)
    d_qkv = jnp.concatenate([dq.reshape(rows, D), dk.reshape(rows, D), dv.reshape(rows, D)], axis=1).astype(jnp.bfloat16)
    grad_qkv = jnp.dot(hb1.T, d_qkv, preferred_element_type=jnp.float32)
    d_h1 = jnp.dot(d_qkv, w_qkv.T, preferred_element_type=jnp.float32)
    d_x1, grad_g1 = norm_back(d_h1, n1, r1, gain_attn)
    return (out, d_mid + d_x1, (grad_qkv, grad_out, grad_in, grad_down, grad_g1, grad_g2))

def reference(tokens, lengths, positions, w_qkv, w_out, w_in, w_down, gain_attn, gain_mlp, cotangent):
    outputs = []
    grads_in = []
    totals = None
    for seq in range(SEQS):
        out, d_x, grads = one_sequence(tokens[seq], lengths[seq], positions[seq], w_qkv, w_out, w_in, w_down, gain_attn, gain_mlp, cotangent[seq])
        outputs.append(out)
        grads_in.append(d_x)
        if totals is None:
            totals = grads
        else:
            totals = tuple((a + b for a, b in zip(totals, grads)))
    return (jnp.stack(outputs), jnp.stack(grads_in), totals[0], totals[1], totals[2], totals[3], totals[4], totals[5])
```

```python
import functools

import jax
import jax.numpy as jnp
from jax import lax
from jax.experimental import pallas as pl
from jax.experimental.pallas import tpu as pltpu
from jax.sharding import PartitionSpec as P

HEADS = 16
HEAD_DIM = 64


eps = 1e-05
theta_base = 160000.0
masked_score = -1e30


def layer_norm(value, gain):
    mean = jnp.mean(value, axis=-1, keepdims=True)
    centered = value - mean
    rstd = lax.rsqrt(jnp.mean(centered * centered, axis=-1, keepdims=True) + eps)
    normed = centered * rstd
    return (normed * gain.astype(jnp.float32), normed, rstd)


def norm_back(grad_h, normed, rstd, gain):
    grad_n = grad_h * gain.astype(jnp.float32)
    grad_gain = jnp.sum(grad_h * normed, axis=0)
    grad_x = rstd * (
        grad_n
        - jnp.mean(grad_n, axis=-1, keepdims=True)
        - normed * jnp.mean(grad_n * normed, axis=-1, keepdims=True)
    )
    return (grad_x, grad_gain)


def rope_tables(pos_ids):
    half = HEAD_DIM // 2
    inverse = theta_base ** (-(jnp.arange(half, dtype=jnp.float32) * (2.0 / HEAD_DIM)))
    angles = pos_ids.astype(jnp.float32)[:, None] * inverse[None, :]
    return (jnp.cos(angles)[:, None, :], jnp.sin(angles)[:, None, :])


def rotate(value, cosv, sinv):
    half = value.shape[-1] // 2
    first, second = (value[..., :half], value[..., half:])
    return jnp.concatenate([first * cosv - second * sinv, second * cosv + first * sinv], axis=-1)


def unrotate(value, cosv, sinv):
    half = value.shape[-1] // 2
    first, second = (value[..., :half], value[..., half:])
    return jnp.concatenate([first * cosv + second * sinv, second * cosv - first * sinv], axis=-1)


def gelu_parts(value):
    cdf = 0.5 * (1.0 + jax.scipy.special.erf(value * 0.7071067811865476))
    dens = jnp.exp(-0.5 * value * value) * 0.3989422804014327
    return (value * cdf, cdf + value * dens)


def block_size(total_rows):
    size = total_rows
    while size > 2048 and size % 2 == 0:
        size = size // 2
    return size


def over_blocks(step, carry, pieces, start):
    total_rows = pieces[0].shape[0]
    size = block_size(total_rows)
    turns = total_rows // size
    if turns == 1:
        return step(carry, pieces, start)

    def one_turn(turn, current):
        parts = tuple((lax.dynamic_slice_in_dim(piece, turn * size, size, 0) for piece in pieces))
        return step(current, parts, start + turn * size)

    return lax.fori_loop(0, turns, one_turn, carry)


def shards(tokens, lengths, positions, w_qkv, w_out, w_in, w_down, gain_attn, gain_mlp, cotangent):
    rows = tokens.shape[1]
    width = tokens.shape[2]
    scale = HEAD_DIM ** (-0.5)
    length = lengths[0]
    hidden_in = tokens[0].astype(jnp.float32)
    full_qkv, full_out, full_in, full_down, full_g1, full_g2 = (
        lax.all_gather(w_qkv, "shard", axis=0, tiled=True),
        lax.all_gather(w_out, "shard", axis=0, tiled=True),
        lax.all_gather(w_in, "shard", axis=0, tiled=True),
        lax.all_gather(w_down, "shard", axis=0, tiled=True),
        lax.all_gather(gain_attn, "shard", axis=0, tiled=True),
        lax.all_gather(gain_mlp, "shard", axis=0, tiled=True),
    )
    hidden_units = full_down.shape[0]
    h1, n1, r1 = layer_norm(hidden_in, full_g1)
    hb1 = h1.astype(jnp.bfloat16)
    qkv = jnp.dot(hb1, full_qkv, preferred_element_type=jnp.float32)
    cosv, sinv = rope_tables(positions[0])
    query_heads = rotate(qkv[:, :width].reshape(rows, HEADS, HEAD_DIM), cosv, sinv).astype(
        jnp.bfloat16
    )
    key_heads = rotate(qkv[:, width : 2 * width].reshape(rows, HEADS, HEAD_DIM), cosv, sinv).astype(
        jnp.bfloat16
    )
    value_heads = qkv[:, 2 * width :].reshape(rows, HEADS, HEAD_DIM).astype(jnp.bfloat16)
    key_rows = key_heads.reshape(rows, width)
    value_rows = value_heads.reshape(rows, width)
    query_rows = query_heads.reshape(rows, width)
    key_start = lax.axis_index("ctx") * rows
    key_valid = key_start + jnp.arange(rows) < length

    def forward_step(carry, pieces, start):
        running, total, accum = carry
        key_piece, value_piece = pieces
        count = key_piece.shape[0]
        key_part = key_piece.reshape(count, HEADS, HEAD_DIM)
        value_part = value_piece.reshape(count, HEADS, HEAD_DIM)
        valid = start + jnp.arange(count) < length
        scores = (
            jnp.einsum("qhd,khd->hqk", query_heads, key_part, preferred_element_type=jnp.float32)
            * scale
        )
        scores = jnp.where(valid, scores, masked_score)
        newest = jnp.maximum(running, jnp.max(scores, axis=-1))
        factor = jnp.exp(running - newest)
        expo = jnp.where(valid, jnp.exp(scores - newest[:, :, None]), 0.0)
        total = total * factor + jnp.sum(expo, axis=-1)
        accum = accum * factor[:, :, None] + jnp.einsum(
            "hqk,khd->hqd",
            expo.astype(jnp.bfloat16),
            value_part,
            preferred_element_type=jnp.float32,
        )
        return (newest, total, accum)

    start_state = (
        jnp.full((HEADS, rows), masked_score, jnp.float32),
        jnp.zeros((HEADS, rows), jnp.float32),
        jnp.zeros((HEADS, rows, HEAD_DIM), jnp.float32),
    )
    running, total, accum = over_blocks(
        forward_step,
        start_state,
        (
            lax.all_gather(key_rows, "ctx", axis=0, tiled=True),
            lax.all_gather(value_rows, "ctx", axis=0, tiled=True),
        ),
        jnp.int32(0),
    )
    attended = jnp.transpose(accum / total[:, :, None], (1, 0, 2))
    lse_local = running + jnp.log(total)
    ob = attended.reshape(rows, width).astype(jnp.bfloat16)
    mid = hidden_in + jnp.dot(ob, full_out, preferred_element_type=jnp.float32)
    h2, n2, r2 = layer_norm(mid, full_g2)
    hb2 = h2.astype(jnp.bfloat16)
    u = jnp.dot(hb2, full_in, preferred_element_type=jnp.float32)
    inp, gate = (u[:, :hidden_units], u[:, hidden_units:])
    gel, dgel = gelu_parts(inp)
    act = (gel * gate).astype(jnp.bfloat16)
    output = (mid + jnp.dot(act, full_down, preferred_element_type=jnp.float32)).astype(
        jnp.bfloat16
    )
    cot_b = cotangent[0]
    d_act = jnp.dot(cot_b, full_down.T, preferred_element_type=jnp.float32)
    d_u = jnp.concatenate([d_act * gate * dgel, d_act * gel], axis=1).astype(jnp.bfloat16)
    d_h2 = jnp.dot(d_u, full_in.T, preferred_element_type=jnp.float32)
    d_x2, grad_g2 = norm_back(d_h2, n2, r2, full_g2)
    d_mid = cot_b.astype(jnp.float32) + d_x2
    d_mid_b = d_mid.astype(jnp.bfloat16)
    grad_rows = jnp.dot(d_mid_b, full_out.T, preferred_element_type=jnp.float32).astype(
        jnp.bfloat16
    )
    grad_heads = grad_rows.reshape(rows, HEADS, HEAD_DIM)
    delta_local = jnp.transpose(jnp.sum(grad_heads.astype(jnp.float32) * attended, axis=-1))
    lse_all, delta_all = (
        lax.all_gather(lse_local, "ctx", axis=1, tiled=True),
        lax.all_gather(delta_local, "ctx", axis=1, tiled=True),
    )

    def query_step(grad_q, pieces, start):
        key_piece, value_piece = pieces
        count = key_piece.shape[0]
        key_part = key_piece.reshape(count, HEADS, HEAD_DIM)
        value_part = value_piece.reshape(count, HEADS, HEAD_DIM)
        valid = start + jnp.arange(count) < length
        scores = (
            jnp.einsum("qhd,khd->hqk", query_heads, key_part, preferred_element_type=jnp.float32)
            * scale
        )
        probs = jnp.where(valid, jnp.exp(scores - lse_local[:, :, None]), 0.0)
        grad_p = jnp.einsum(
            "qhd,khd->hqk", grad_heads, value_part, preferred_element_type=jnp.float32
        )
        grad_s = (probs * (grad_p - delta_local[:, :, None])).astype(jnp.bfloat16)
        return grad_q + jnp.einsum(
            "hqk,khd->qhd", grad_s, key_part, preferred_element_type=jnp.float32
        )

    def key_step(carry, pieces, start):
        grad_k, grad_v = carry
        query_piece, grad_piece = pieces
        count = query_piece.shape[0]
        query_part = query_piece.reshape(count, HEADS, HEAD_DIM)
        grad_part = grad_piece.reshape(count, HEADS, HEAD_DIM)
        lse_part = lax.dynamic_slice_in_dim(lse_all, start, count, 1)
        delta_part = lax.dynamic_slice_in_dim(delta_all, start, count, 1)
        scores = (
            jnp.einsum("qhd,khd->hqk", query_part, key_heads, preferred_element_type=jnp.float32)
            * scale
        )
        probs = jnp.where(key_valid, jnp.exp(scores - lse_part[:, :, None]), 0.0)
        grad_v = grad_v + jnp.einsum(
            "hqk,qhd->khd",
            probs.astype(jnp.bfloat16),
            grad_part,
            preferred_element_type=jnp.float32,
        )
        grad_p = jnp.einsum(
            "qhd,khd->hqk", grad_part, value_heads, preferred_element_type=jnp.float32
        )
        grad_s = (probs * (grad_p - delta_part[:, :, None])).astype(jnp.bfloat16)
        grad_k = grad_k + jnp.einsum(
            "hqk,qhd->khd", grad_s, query_part, preferred_element_type=jnp.float32
        )
        return (grad_k, grad_v)

    zero_heads = jnp.zeros((rows, HEADS, HEAD_DIM), jnp.float32)
    grad_q = over_blocks(
        query_step,
        zero_heads,
        (
            lax.all_gather(key_rows, "ctx", axis=0, tiled=True),
            lax.all_gather(value_rows, "ctx", axis=0, tiled=True),
        ),
        jnp.int32(0),
    )
    grad_k, grad_v = over_blocks(
        key_step,
        (zero_heads, zero_heads),
        (
            lax.all_gather(query_rows, "ctx", axis=0, tiled=True),
            lax.all_gather(grad_rows, "ctx", axis=0, tiled=True),
        ),
        jnp.int32(0),
    )
    grad_q = unrotate(grad_q * scale, cosv, sinv)
    grad_k = unrotate(grad_k * scale, cosv, sinv)
    d_qkv = jnp.concatenate(
        [grad_q.reshape(rows, width), grad_k.reshape(rows, width), grad_v.reshape(rows, width)],
        axis=1,
    ).astype(jnp.bfloat16)
    d_h1 = jnp.dot(d_qkv, full_qkv.T, preferred_element_type=jnp.float32)
    d_x1, grad_g1 = norm_back(d_h1, n1, r1, full_g1)
    grad_tokens = d_mid + d_x1
    grad_qkv = jnp.dot(hb1.T, d_qkv, preferred_element_type=jnp.float32)
    grad_out = jnp.dot(ob.T, d_mid_b, preferred_element_type=jnp.float32)
    grad_in = jnp.dot(hb2.T, d_u, preferred_element_type=jnp.float32)
    grad_down = jnp.dot(act.T, cot_b, preferred_element_type=jnp.float32)
    shares = (
        lax.psum_scatter(grad_qkv, "shard", scatter_dimension=0, tiled=True),
        lax.psum_scatter(grad_out, "shard", scatter_dimension=0, tiled=True),
        lax.psum_scatter(grad_in, "shard", scatter_dimension=0, tiled=True),
        lax.psum_scatter(grad_down, "shard", scatter_dimension=0, tiled=True),
        lax.psum_scatter(grad_g1, "shard", scatter_dimension=0, tiled=True),
        lax.psum_scatter(grad_g2, "shard", scatter_dimension=0, tiled=True),
    )
    summed = lax.psum((shares[0], shares[1], shares[2], shares[3], shares[4], shares[5]), "ctx")
    return (
        output.reshape(1, rows, width),
        grad_tokens.reshape(1, rows, width),
        summed[0],
        summed[1],
        summed[2],
        summed[3],
        summed[4],
        summed[5],
    )


MESH = pl.DeviceIdType.MESH
F32 = jnp.float32
BF16 = jnp.bfloat16
CTX = 16


def fast_fits(mesh):
    return mesh.shape["ctx"] == CTX and mesh.shape["shard"] == 2


def place():
    me = lax.axis_index("ctx")
    return me, me // 4, (me // 2) % 2, me % 2


def at(z, x, c):
    return {"ctx": z * 4 + x * 2 + c}


def when(cond, body):
    if cond is True:
        body()
    else:
        pl.when(cond)(body)


def both(a, b):
    if a is True:
        return b
    if b is True:
        return a
    return jnp.logical_and(a, b)


def gather_kernel(sources, count, *refs):
    ins, outs = refs[:count], refs[count : 2 * count]
    local_sem, send_sem, recv_sem = refs[2 * count :]
    me, z, x, c = place()
    y = lax.axis_index("shard")
    up, down = z < 3, z > 0
    barrier = pltpu.get_barrier_semaphore()
    when(up, lambda: pl.semaphore_signal(barrier, 1, device_id=at(z + 1, x, c), device_id_type=MESH))
    when(down, lambda: pl.semaphore_signal(barrier, 1, device_id=at(z - 1, x, c), device_id_type=MESH))
    pl.semaphore_signal(barrier, 1, device_id=at(z, 1 - x, c), device_id_type=MESH)
    pl.semaphore_signal(barrier, 1, device_id=at(z, x, 1 - c), device_id_type=MESH)
    pl.semaphore_wait(barrier, 2 + up.astype(jnp.int32) + down.astype(jnp.int32))
    targets = (at(z + 1, x, c), at(z - 1, x, c), at(z, 1 - x, c), at(z, x, 1 - c))

    def has(a, zo):
        return sources[a](zo, y)

    def copy(a, src, origin, way):
        return pltpu.make_async_remote_copy(
            src_ref=src,
            dst_ref=outs[a].at[origin],
            send_sem=send_sem.at[a, way, origin],
            recv_sem=recv_sem.at[a, origin],
            device_id=targets[way],
            device_id_type=MESH,
        )

    def got(a, origin):
        copy(a, ins[a], origin, 3).wait_recv()

    def own(a):
        def go():
            pltpu.make_async_copy(ins[a], outs[a].at[me], local_sem.at[a]).start()
            when(up, lambda: copy(a, ins[a], me, 0).start())
            when(down, lambda: copy(a, ins[a], me, 1).start())
            copy(a, ins[a], me, 2).start()
            copy(a, ins[a], me, 3).start()

        when(has(a, z), go)

    for a in range(count):
        own(a)
    for d in (1, 2, 3):
        for a in range(count):

            def below(a=a, zo=z - d):
                origin = zo * 4 + x * 2 + c
                got(a, origin)
                when(up, lambda: copy(a, outs[a].at[origin], origin, 0).start())
                copy(a, outs[a].at[origin], origin, 2).start()
                copy(a, outs[a].at[origin], origin, 3).start()

            def above(a=a, zo=z + d):
                origin = zo * 4 + x * 2 + c
                got(a, origin)
                when(down, lambda: copy(a, outs[a].at[origin], origin, 1).start())
                copy(a, outs[a].at[origin], origin, 2).start()
                copy(a, outs[a].at[origin], origin, 3).start()

            when(both(has(a, z - d), z - d >= 0), below)
            when(both(has(a, z + d), z + d <= 3), above)
    for k in range(4):
        zo = lax.rem(z + k, 4)
        origin = zo * 4 + (1 - x) * 2 + c
        for a in range(count):

            def across(a=a, origin=origin):
                got(a, origin)
                copy(a, outs[a].at[origin], origin, 3).start()

            when(has(a, zo), across)
    for k in range(8):
        zo = k // 2
        for a in range(count):
            when(has(a, zo), lambda a=a, k=k: got(a, k * 2 + 1 - c))
    for a in range(count):
        when(has(a, z), lambda a=a: pltpu.make_async_copy(ins[a], outs[a].at[me], local_sem.at[a]).wait())
        for zo in range(4):
            origin = zo * 4 + x * 2 + c
            other = zo * 4 + (1 - x) * 2 + c

            def drain(a=a, zo=zo, origin=origin, other=other):
                when(both(up, zo <= z), lambda: copy(a, ins[a], origin, 0).wait_send())
                when(both(down, zo >= z), lambda: copy(a, ins[a], origin, 1).wait_send())
                copy(a, ins[a], origin, 2).wait_send()
                copy(a, ins[a], origin, 3).wait_send()
                copy(a, ins[a], other, 3).wait_send()

            when(has(a, zo), drain)


def everywhere(zo, y):
    return True


def gather(arrays, cid, name, sources=None):
    count = len(arrays)
    sources = sources or (everywhere,) * count
    kernel = functools.partial(gather_kernel, sources, count)
    hbm = pl.BlockSpec(memory_space=pl.ANY)
    return pl.pallas_call(
        kernel,
        out_shape=[jax.ShapeDtypeStruct((CTX,) + a.shape, a.dtype) for a in arrays],
        in_specs=[hbm] * count,
        out_specs=[hbm] * count,
        scratch_shapes=[
            pltpu.SemaphoreType.DMA((count,)),
            pltpu.SemaphoreType.DMA((count, 4, CTX)),
            pltpu.SemaphoreType.DMA((count, CTX)),
        ],
        compiler_params=pltpu.CompilerParams(collective_id=cid, has_side_effects=True),
        name=name,
    )(*arrays)


def exchange_kernel(peers, spread, in_ref, out_ref, local_sem, send_sem, recv_sem):
    members, mine = peers()
    size = len(members)
    barrier = pltpu.get_barrier_semaphore()
    for k in range(1, size):
        pl.semaphore_signal(barrier, 1, device_id={"ctx": members[k][0]}, device_id_type=MESH)
    pl.semaphore_wait(barrier, size - 1)

    def source(slot):
        return in_ref if spread else in_ref.at[slot]

    def copy(k, dst):
        device, slot = members[k]
        return pltpu.make_async_remote_copy(
            src_ref=source(slot),
            dst_ref=out_ref.at[dst],
            send_sem=send_sem.at[k],
            recv_sem=recv_sem.at[dst],
            device_id={"ctx": device},
            device_id_type=MESH,
        )

    local = pltpu.make_async_copy(source(mine), out_ref.at[mine], local_sem)
    for k in range(1, size):
        copy(k, mine).start()
    local.start()
    local.wait()
    for k in range(1, size):
        arrived = copy(k, members[k][1])
        arrived.wait_recv()
        arrived.wait_send()


def exchange(array, peers, size, cid, name, spread=False):
    shape = ((size,) + array.shape) if spread else array.shape
    hbm = pl.BlockSpec(memory_space=pl.ANY)
    return pl.pallas_call(
        functools.partial(exchange_kernel, peers, spread),
        out_shape=jax.ShapeDtypeStruct(shape, array.dtype),
        in_specs=[hbm],
        out_specs=hbm,
        scratch_shapes=[
            pltpu.SemaphoreType.DMA,
            pltpu.SemaphoreType.DMA((size,)),
            pltpu.SemaphoreType.DMA((size,)),
        ],
        compiler_params=pltpu.CompilerParams(collective_id=cid, has_side_effects=True),
        name=name,
    )(array)


def all_peers():
    me = lax.axis_index("ctx")
    return [(lax.rem(me + k, CTX), lax.rem(me + k, CTX)) for k in range(CTX)], me


def square_peers():
    me, z, x, c = place()
    corner, zp = (z // 2) * 2, z % 2
    members = []
    for dz, dx in ((0, 0), (0, 1), (1, 0), (1, 1)):
        oz, ox = (zp + dz) % 2, (x + dx) % 2
        members.append(((corner + oz) * 4 + ox * 2 + c, oz * 2 + ox))
    return members, zp * 2 + x


BQ = 256


def attend_kernel(len_ref, k_ref, q_ref, v_ref, o_ref, lse_ref):
    total_keys = k_ref.shape[0]
    length = len_ref[0]
    valid = lax.broadcasted_iota(jnp.int32, (total_keys, BQ), 0) < length

    def step(i, carry):
        cols = pl.ds(pl.multiple_of(i * BQ, BQ), BQ)
        s = jnp.dot(k_ref[...], q_ref[:, cols], preferred_element_type=F32)
        s = jnp.where(valid, s, masked_score)
        top = jnp.max(s, axis=0, keepdims=True)
        e = jnp.exp(s - top)
        tot = jnp.sum(e, axis=0, keepdims=True)
        acc = jnp.dot(v_ref[...], e.astype(BF16), preferred_element_type=F32)
        o_ref[:, cols] = acc / tot
        lse_ref[:, cols] = top + jnp.log(tot)
        return carry

    lax.fori_loop(0, total_keys // BQ, step, 0)


def attend(length, k_nat, q_t, v_t):
    keys = k_nat.shape[0]
    vmem = pl.BlockSpec(memory_space=pltpu.VMEM)
    return pl.pallas_call(
        attend_kernel,
        out_shape=(
            jax.ShapeDtypeStruct((HEAD_DIM, keys), F32),
            jax.ShapeDtypeStruct((1, keys), F32),
        ),
        in_specs=[pl.BlockSpec(memory_space=pltpu.SMEM), vmem, vmem, vmem],
        out_specs=(vmem, vmem),
        name="attend",
    )(length, k_nat, q_t, v_t)


def attend_back_kernel(
    len_ref, k_ref, v_ref, kt_ref, q_ref, qn_ref, do_ref, don_ref, lse_ref, delta_ref, dq_ref, dk_ref, dv_ref
):
    total_keys = k_ref.shape[0]
    length = len_ref[0]
    valid = lax.broadcasted_iota(jnp.int32, (total_keys, BQ), 0) < length
    dk_ref[...] = jnp.zeros_like(dk_ref)
    dv_ref[...] = jnp.zeros_like(dv_ref)

    def step(i, carry):
        cols = pl.ds(pl.multiple_of(i * BQ, BQ), BQ)
        s = jnp.dot(k_ref[...], q_ref[:, cols], preferred_element_type=F32)
        p = jnp.where(valid, jnp.exp(s - lse_ref[:, cols]), 0.0)
        dp = jnp.dot(v_ref[...], do_ref[:, cols], preferred_element_type=F32)
        ds = (p * (dp - delta_ref[:, cols])).astype(BF16)
        dq_ref[:, cols] = jnp.dot(kt_ref[...], ds, preferred_element_type=F32)
        dk_ref[...] += jnp.dot(ds, qn_ref[cols, :], preferred_element_type=F32)
        dv_ref[...] += jnp.dot(p.astype(BF16), don_ref[cols, :], preferred_element_type=F32)
        return carry

    lax.fori_loop(0, total_keys // BQ, step, 0)


def attend_back(length, k_nat, v_nat, k_t, q_t, q_nat, do_t, do_nat, lse, delta):
    keys = k_nat.shape[0]
    vmem = pl.BlockSpec(memory_space=pltpu.VMEM)
    return pl.pallas_call(
        attend_back_kernel,
        out_shape=(
            jax.ShapeDtypeStruct((HEAD_DIM, keys), F32),
            jax.ShapeDtypeStruct((keys, HEAD_DIM), F32),
            jax.ShapeDtypeStruct((keys, HEAD_DIM), F32),
        ),
        in_specs=[pl.BlockSpec(memory_space=pltpu.SMEM)] + [vmem] * 9,
        out_specs=(vmem, vmem, vmem),
        name="attend_back",
    )(length, k_nat, v_nat, k_t, q_t, q_nat, do_t, do_nat, lse, delta)


def contract(a, b, da, db):
    return lax.dot_general(a, b, (((da,), (db,)), ((), ())), preferred_element_type=F32)


def turn(v, cos_t, sin_t, sign):
    half = HEAD_DIM // 2
    a, b = v[:half], v[half:]
    return jnp.concatenate([a * cos_t - sign * b * sin_t, b * cos_t + sign * a * sin_t], axis=0)


def fast_shards(tokens, lengths, positions, w_qkv, w_out, w_in, w_down, gain_attn, gain_mlp, cotangent):
    rows, width = tokens.shape[1], tokens.shape[2]
    length_all = rows * CTX
    half = width // 2
    hidden = w_down.shape[0] * 2
    block = hidden // 4
    sub = block // 2
    scale = HEAD_DIM ** (-0.5)
    me, z, x, c = place()
    y = lax.axis_index("shard")
    group, pair = z // 2, (z % 2) * 2 + x

    def swap(v):
        return lax.ppermute(v, "shard", [(0, 1), (1, 0)])

    def sibling(v):
        return lax.ppermute(v, "ctx", [(i, i ^ 1) for i in range(CTX)])

    def ordered(mine, other, axis):
        return jnp.where(
            y == 0,
            jnp.concatenate([mine, other], axis=axis),
            jnp.concatenate([other, mine], axis=axis),
        )

    def my_half(v, which, axis):
        size = v.shape[axis] // 2
        return lax.dynamic_slice_in_dim(v, which * size, size, axis)

    gains = jnp.stack([gain_attn, gain_mlp])
    gains = ordered(gains, swap(gains), 1)
    g1, g2 = gains[0], gains[1]
    wh = lax.dynamic_slice(w_qkv.reshape(half, 3, width), (0, 0, HEAD_DIM * me), (half, 3, HEAD_DIM))
    wh = wh.reshape(half, 3 * HEAD_DIM).T
    wh = ordered(wh, swap(wh), 1)
    hidden_in = tokens[0].astype(F32)
    h1, n1, r1 = layer_norm(hidden_in, g1)
    hb1 = h1.astype(BF16)
    (hb1_all, pos_all) = gather([hb1, positions.astype(F32)], 0, "gather_tokens")
    hb1_all = hb1_all.reshape(length_all, width)
    pos_all = pos_all.reshape(length_all)
    hd2 = HEAD_DIM // 2
    inverse = theta_base ** (-(jnp.arange(hd2, dtype=F32) * (2.0 / HEAD_DIM)))
    angles = inverse[:, None] * pos_all[None, :]
    cos_t, sin_t = jnp.cos(angles), jnp.sin(angles)
    qkv_t = contract(wh, hb1_all, 1, 1)
    q_t = turn(qkv_t[:HEAD_DIM], cos_t, sin_t, 1.0).astype(BF16)
    k_t = turn(qkv_t[HEAD_DIM : 2 * HEAD_DIM], cos_t, sin_t, 1.0).astype(BF16)
    v_t = qkv_t[2 * HEAD_DIM :].astype(BF16)
    qs_t = q_t * jnp.asarray(scale, BF16)
    k_nat, v_nat = k_t.T, v_t.T
    o_t, lse = attend(lengths, k_nat, qs_t, v_t)
    ob_h = o_t.astype(BF16)

    def pieces(v):
        return jnp.transpose(v.reshape(v.shape[0], CTX, rows), (1, 0, 2))

    ob_t = exchange(pieces(ob_h), all_peers, CTX, 1, "spread_attended").reshape(width, rows)
    w_out_all = ordered(w_out, swap(w_out), 0)
    mid = hidden_in + contract(ob_t, w_out_all, 0, 0)
    h2, n2, r2 = layer_norm(mid, g2)
    hb2 = h2.astype(BF16)
    cot_b = cotangent[0]
    w_in3 = lax.dynamic_slice(w_in.reshape(half, 2, hidden), (0, c, block * pair), (half, 1, block))
    w_in_half = w_in3.reshape(half, block).T
    w_in_one = ordered(w_in_half, swap(w_in_half), 1)
    w_in_two = sibling(w_in_one)
    w_in_t = jnp.where(
        c == 0, jnp.concatenate([w_in_one, w_in_two], 0), jnp.concatenate([w_in_two, w_in_one], 0)
    )
    owner = pair // 2
    wd_local = lax.dynamic_slice(w_down, (block * (pair % 2) + sub * c, 0), (sub, width))
    wd_one = jnp.where(owner == y, wd_local, swap(wd_local))
    wd_two = sibling(wd_one)
    wd = jnp.where(c == 0, jnp.concatenate([wd_one, wd_two], 0), jnp.concatenate([wd_two, wd_one], 0))
    both_all = exchange(jnp.stack([hb2, cot_b]), square_peers, 4, 2, "gather_square", spread=True)
    hb2_all = both_all[:, 0].reshape(4 * rows, width)
    cot_all = both_all[:, 1].reshape(4 * rows, width)
    u_t = contract(w_in_t, hb2_all, 1, 1)
    inp, gate = u_t[:block], u_t[block:]
    gel, dgel = gelu_parts(inp)
    act_t = (gel * gate).astype(BF16)
    d_act = contract(wd, cot_all, 1, 1)
    d_u_t = jnp.concatenate([d_act * gate * dgel, d_act * gel], axis=0).astype(BF16)
    d_h2_part = contract(d_u_t, w_in_t, 0, 0)
    out_part = contract(act_t, wd, 0, 0)
    parts = jnp.stack([d_h2_part, out_part]).astype(BF16).reshape(2, 4, rows, width)
    parts = exchange(jnp.transpose(parts, (1, 0, 2, 3)), square_peers, 4, 3, "sum_square")
    sums = jnp.sum(parts.astype(F32), axis=0)
    d_h2 = sums[0]
    output = (mid + sums[1]).astype(BF16)
    gi = contract(d_u_t, hb2_all, 1, 0)
    gd = contract(act_t, cot_all, 1, 0)
    gi = my_half(gi, c, 0) + sibling(my_half(gi, 1 - c, 0).astype(BF16)).astype(F32)
    gd = my_half(gd, c, 1) + sibling(my_half(gd, 1 - c, 1).astype(BF16)).astype(F32)
    gi = my_half(gi, y, 1) + swap(my_half(gi, 1 - y, 1).astype(BF16)).astype(F32)
    gd = gd + swap(gd.astype(BF16)).astype(F32)

    def far(v):
        return lax.ppermute(v, "ctx", [(i, (i + 8) % CTX) for i in range(CTX)])

    gi = my_half(gi, group, 0) + far(my_half(gi, 1 - group, 0).astype(BF16)).astype(F32)
    gd = my_half(gd, group, 0) + far(my_half(gd, 1 - group, 0).astype(BF16)).astype(F32)
    gi, gd = gi.astype(BF16), gd.astype(BF16)
    d_x2, gg2 = norm_back(d_h2, n2, r2, g2)
    d_mid = cot_b.astype(F32) + d_x2
    d_mid_b = d_mid.astype(BF16)
    (d_mid_all,) = gather([d_mid_b], 4, "gather_d_mid")
    d_mid_all = d_mid_all.reshape(length_all, width)
    wo_h = lax.dynamic_slice(w_out_all, (HEAD_DIM * me, 0), (HEAD_DIM, width))
    do_t = contract(wo_h, d_mid_all, 1, 1).astype(BF16)
    delta = jnp.sum(do_t.astype(F32) * o_t, axis=0, keepdims=True)
    dq_t, dk, dv = attend_back(lengths, k_nat, v_nat, k_t, qs_t, q_t.T, do_t, do_t.T, lse, delta)
    dq_t = turn(dq_t * scale, cos_t, sin_t, -1.0)
    dk_t = turn(dk.T * scale, cos_t, sin_t, -1.0)
    d_qkv_t = jnp.concatenate([dq_t, dk_t, dv.T], axis=0).astype(BF16)
    d_qkv = exchange(pieces(d_qkv_t), all_peers, CTX, 5, "spread_d_qkv")
    d_qkv = jnp.transpose(d_qkv.reshape(CTX, 3, HEAD_DIM, rows), (1, 0, 2, 3)).reshape(3 * width, rows)
    w_qkv_other = sibling(swap(my_half(w_qkv, c, 0)))
    w_qkv_mine = swap(my_half(w_qkv, c, 0))
    w_qkv_swap = jnp.where(
        c == 0,
        jnp.concatenate([w_qkv_mine, w_qkv_other], 0),
        jnp.concatenate([w_qkv_other, w_qkv_mine], 0),
    )
    d_h1 = ordered(contract(d_qkv, w_qkv, 0, 1), contract(d_qkv, w_qkv_swap, 0, 1), 1)
    d_x1, gg1 = norm_back(d_h1, n1, r1, g1)
    grad_tokens = d_mid + d_x1
    gq = contract(d_qkv_t, hb1_all, 1, 0)
    go = contract(ob_h, d_mid_all, 1, 0)
    gq = (my_half(gq, y, 1) + swap(my_half(gq, 1 - y, 1).astype(BF16)).astype(F32)).astype(BF16)
    go = (go + swap(go.astype(BF16)).astype(F32)).astype(BF16)
    gg = jnp.stack([gg1, gg2])
    gg = my_half(gg, y, 1) + swap(my_half(gg, 1 - y, 1))
    gq_all, go_all, gi_all, gd_all, gg_all = gather(
        [gq, go, gi, gd, gg],
        6,
        "gather_grads",
        (
            everywhere,
            lambda zo, y: zo // 2 == y,
            everywhere,
            lambda zo, y: zo % 2 == y,
            everywhere,
        ),
    )
    grad_qkv = jnp.transpose(gq_all.reshape(CTX, 3, HEAD_DIM, half), (3, 1, 0, 2)).reshape(half, 3 * width)
    grad_out = lax.dynamic_slice_in_dim(go_all, y * 8, 8, 0).reshape(half, width)
    gi_all = gi_all.reshape(2, 2, 2, 2, sub, half)
    grad_in = jnp.transpose(gi_all, (5, 3, 1, 2, 0, 4)).reshape(half, 2 * hidden)
    gd_all = gd_all.reshape(2, 2, 2, 2, sub, half)
    gd_all = lax.dynamic_index_in_dim(gd_all, y, 1, keepdims=False)
    grad_down = jnp.transpose(gd_all, (1, 0, 3, 2, 4)).reshape(hidden // 2, width)
    gg_sum = jnp.sum(gg_all, axis=0)
    return (
        output.reshape(1, rows, width),
        grad_tokens.reshape(1, rows, width),
        grad_qkv.astype(F32),
        grad_out.astype(F32),
        grad_in.astype(F32),
        grad_down.astype(F32),
        gg_sum[0],
        gg_sum[1],
    )


def solution(mesh):
    in_specs = (
        P("shard", "ctx", None),
        P("shard"),
        P("shard", "ctx"),
        P("shard", None),
        P("shard", None),
        P("shard", None),
        P("shard", None),
        P("shard"),
        P("shard"),
        P("shard", "ctx", None),
    )
    out_specs = (
        P("shard", "ctx", None),
        P("shard", "ctx", None),
        P("shard", None),
        P("shard", None),
        P("shard", None),
        P("shard", None),
        P("shard"),
        P("shard"),
    )
    plan = fast_shards if fast_fits(mesh) else shards
    return jax.shard_map(plan, mesh=mesh, in_specs=in_specs, out_specs=out_specs, check_vma=False)
```
